32 devices in a mesh: dp: 4 (over y, z), ep: 8 (over x, core).
Axes of the slice: x: 4, y: 2, z: 2, core: 2. Of those that a mesh axis runs over, the one named last changes fastest.
The devices are a block of a 4x4x8 slice.
Arguments:
- x_in: bfloat16 [384, 384, 768], P(('dp', 'ep')), parts along dimension 0
- pad_mask: int32 [384, 384], P(('dp', 'ep')), parts along dimension 0
- rel_bias: float32 [12, 384, 384], replicated
- expert_idx: int32 [2, 384, 384], P(None, ('dp', 'ep')), parts along dimension 1
- norm_scale: float32 [2, 2, 768], replicated
- w_query: bfloat16 [2, 768, 768], replicated
- w_key: bfloat16 [2, 768, 768], replicated
- w_value: bfloat16 [2, 768, 768], replicated
- w_attn_out: bfloat16 [2, 768, 768], replicated
- w_router: float32 [2, 768, 32], replicated
- w_in: bfloat16 [2, 32, 768, 3072], P(None, 'ep')
- w_out: bfloat16 [2, 32, 3072, 768], P(None, 'ep')
Outputs:
- output: bfloat16 [384, 384, 768], P(('dp', 'ep')), parts along dimension 0
There are 4 independent parts. The reference program is written for one: setup_inputs(seed, part) draws one part's arguments, and reference() takes and returns one part's arrays. A program takes and returns all parts, laid end to end along the dimension named above; an argument that names none is the same for every part.
All inputs are finite; a program needn't handle non-finite values.
Results may differ from the reference program's by a relative error of at most 0.0195101.
Values are sent between devices in bfloat16 or wider.
A program may use at most 768 MiB of HBM per device.

```python
import jax
import jax.numpy as jnp
from jax import lax

SEQS = 12
SEQ = 384
D = 768
HEADS = 12
HEAD = 64
FF = 3072
EXPERTS = 32
GROUPS = 8
CAP_FACTOR = 2
NORM_EPS = 1e-6
NEG_BIG = -1e9
TOKENS = SEQS * SEQ
NUM_SEQ = GROUPS * SEQS
INNER = HEADS * HEAD
CAPACITY = (CAP_FACTOR * TOKENS + EXPERTS - 1) // EXPERTS


def draw_mask(rng_key, num_seq):
    lengths = jax.random.randint(rng_key, (num_seq,), SEQ // 4, SEQ + 1)
    return (jnp.arange(SEQ)[None, :] < lengths[:, None]).astype(jnp.int32)


def draw_routes(rng_key, num_seq):
    route_keys = jax.random.split(rng_key, 5)
    rank_draws = [jax.random.randint(route_keys[draw_id], (2, num_seq, SEQ), 0, EXPERTS) for draw_id in range(3)]
    ranks = jnp.minimum(jnp.minimum(rank_draws[0], rank_draws[1]), rank_draws[2])
    perm_first = jax.random.permutation(route_keys[3], EXPERTS)
    perm_second = jax.random.permutation(route_keys[4], EXPERTS)
    return jnp.stack([perm_first[ranks[0]], perm_second[ranks[1]]]).astype(jnp.int32)


def setup_inputs(seed: int = 0, part: int = 0) -> dict:
    base_key = jax.random.key(seed)
    part_keys = jax.random.split(jax.random.fold_in(base_key, part), 3)
    shared_keys = jax.random.split(base_key, 10)
    x_in = jax.random.normal(part_keys[0], (NUM_SEQ, SEQ, D), jnp.float32).astype(jnp.bfloat16)
    pad_mask = draw_mask(part_keys[1], NUM_SEQ)
    expert_idx = draw_routes(part_keys[2], NUM_SEQ)
    rel_bias = 2.0 * jax.random.normal(shared_keys[0], (HEADS, SEQ, SEQ), jnp.float32)
    norm_scale = jax.random.uniform(shared_keys[1], (2, 2, D), jnp.float32, 0.5, 1.5)
    qk_std = (2.0 / D) ** 0.5 * HEAD ** -0.25
    w_query = (qk_std * jax.random.normal(shared_keys[2], (2, D, INNER), jnp.float32)).astype(jnp.bfloat16)
    w_key = (qk_std * jax.random.normal(shared_keys[3], (2, D, INNER), jnp.float32)).astype(jnp.bfloat16)
    w_value = (D ** -0.5 * jax.random.normal(shared_keys[4], (2, D, INNER), jnp.float32)).astype(jnp.bfloat16)
    w_attn_out = (INNER ** -0.5 * jax.random.normal(shared_keys[5], (2, INNER, D), jnp.float32)).astype(jnp.bfloat16)
    w_router = D ** -0.5 * jax.random.normal(shared_keys[6], (2, D, EXPERTS), jnp.float32)
    w_in = (D ** -0.5 * jax.random.normal(shared_keys[7], (2, EXPERTS, D, FF), jnp.float32)).astype(jnp.bfloat16)
    w_out = (EXPERTS * FF ** -0.5 * jax.random.normal(shared_keys[8], (2, EXPERTS, FF, D), jnp.float32)).astype(jnp.bfloat16)
    return dict(x_in=x_in, pad_mask=pad_mask, rel_bias=rel_bias, expert_idx=expert_idx, norm_scale=norm_scale, w_query=w_query, w_key=w_key, w_value=w_value, w_attn_out=w_attn_out, w_router=w_router, w_in=w_in, w_out=w_out)


def rms_norm(hidden, gain):
    hid32 = hidden.astype(jnp.float32)
    return hid32 * lax.rsqrt(jnp.mean(hid32 * hid32, axis=-1, keepdims=True) + NORM_EPS) * gain


def attention_block(hidden, pad_mask, rel_bias, gain, query_w, key_w, value_w, out_w):
    def one_sequence(seq_pair):
        seq_rows, seq_mask = seq_pair
        normed = rms_norm(seq_rows, gain).astype(jnp.bfloat16)
        query_rows = jnp.dot(normed, query_w, preferred_element_type=jnp.float32).astype(jnp.bfloat16).reshape(SEQ, HEADS, HEAD)
        key_rows = jnp.dot(normed, key_w, preferred_element_type=jnp.float32).astype(jnp.bfloat16).reshape(SEQ, HEADS, HEAD)
        value_rows = jnp.dot(normed, value_w, preferred_element_type=jnp.float32).astype(jnp.bfloat16).reshape(SEQ, HEADS, HEAD)
        scores = jnp.einsum('qhd,khd->hqk', query_rows.astype(jnp.float32), key_rows.astype(jnp.float32))
        scores = scores + rel_bias + jnp.where(seq_mask > 0, 0.0, NEG_BIG)[None, None, :]
        attn_probs = jax.nn.softmax(scores, axis=-1).astype(jnp.bfloat16)
        context = jnp.einsum('hqk,khd->qhd', attn_probs.astype(jnp.float32), value_rows.astype(jnp.float32))
        context = context.astype(jnp.bfloat16).reshape(SEQ, INNER)
        attn_out = jnp.dot(context, out_w, preferred_element_type=jnp.float32)
        return (seq_rows.astype(jnp.float32) + attn_out).astype(jnp.bfloat16)
    return lax.map(one_sequence, (hidden, pad_mask))


def expert_block(hidden, layer_ids, gain, route_w, up_w, down_w):
    grouped = hidden.reshape(GROUPS, TOKENS, D)
    ids_grouped = layer_ids.reshape(GROUPS, TOKENS)

    def route_group(grp_pair):
        grp_rows, grp_ids = grp_pair
        normed32 = rms_norm(grp_rows, gain)
        logits = jnp.dot(normed32, route_w, preferred_element_type=jnp.float32)
        gate_val = jnp.take_along_axis(jax.nn.softmax(logits, axis=-1), grp_ids[:, None], axis=1)[:, 0]
        one_hot = (grp_ids[:, None] == jnp.arange(EXPERTS)[None, :]).astype(jnp.int32)
        token_slot = jnp.take_along_axis(jnp.cumsum(one_hot, axis=0), grp_ids[:, None], axis=1)[:, 0] - 1
        flat_slot = jnp.where(token_slot < CAPACITY, grp_ids * CAPACITY + token_slot, EXPERTS * CAPACITY)
        slot_token = jnp.full((EXPERTS * CAPACITY,), TOKENS, jnp.int32).at[flat_slot].set(jnp.arange(TOKENS, dtype=jnp.int32), mode='drop')
        packed = jnp.take(normed32.astype(jnp.bfloat16), slot_token, axis=0, mode='fill', fill_value=0)
        return packed.reshape(EXPERTS, CAPACITY, D), gate_val, flat_slot

    packed, gate_val, flat_slot = lax.map(route_group, (grouped, ids_grouped))

    def one_expert(expert_parts):
        exp_rows, exp_up, exp_down = expert_parts
        flat_rows = exp_rows.reshape(GROUPS * CAPACITY, D)
        inner_act = jnp.maximum(jnp.dot(flat_rows, exp_up, preferred_element_type=jnp.float32), 0.0).astype(jnp.bfloat16)
        return jnp.dot(inner_act, exp_down, preferred_element_type=jnp.float32).astype(jnp.bfloat16).reshape(GROUPS, CAPACITY, D)

    expert_rows = lax.map(one_expert, (jnp.swapaxes(packed, 0, 1), up_w, down_w))
    expert_rows = jnp.swapaxes(expert_rows, 0, 1).reshape(GROUPS, EXPERTS * CAPACITY, D)

    def combine(grp_parts):
        grp_rows, grp_out, grp_gate, grp_flat = grp_parts
        returned = jnp.take(grp_out, grp_flat, axis=0, mode='fill', fill_value=0)
        return (grp_rows.astype(jnp.float32) + grp_gate[:, None] * returned.astype(jnp.float32)).astype(jnp.bfloat16)

    return lax.map(combine, (grouped, expert_rows, gate_val, flat_slot)).reshape(NUM_SEQ, SEQ, D)


def reference(x_in, pad_mask, rel_bias, expert_idx, norm_scale, w_query, w_key, w_value, w_attn_out, w_router, w_in, w_out):
    def layer_step(hidden, layer_params):
        gains, query_w, key_w, value_w, out_w, route_w, up_w, down_w, layer_ids = layer_params
        hidden = attention_block(hidden, pad_mask, rel_bias, gains[0], query_w, key_w, value_w, out_w)
        hidden = expert_block(hidden, layer_ids, gains[1], route_w, up_w, down_w)
        return hidden, None
    final_state = lax.scan(layer_step, x_in, (norm_scale, w_query, w_key, w_value, w_attn_out, w_router, w_in, w_out, expert_idx))
    return final_state[0]
```

```python
import functools

import jax
import jax.numpy as jnp
from jax import lax
from jax.experimental import pallas as pl
from jax.experimental.pallas import tpu as pltpu
from jax.sharding import PartitionSpec as P

NORM_EPS = 1e-6
NEG_BIG = -1e9
CAP_FACTOR = 2
LANES = 128
MESH = pl.DeviceIdType.MESH
f32 = jnp.float32
bf16 = jnp.bfloat16


def routing_kernel(capacity, ids_ref, place_ref, token_ref):
    num_experts = token_ref.shape[1]
    tok_count = ids_ref.shape[2]
    expert = lax.broadcasted_iota(jnp.int32, (num_experts, LANES), 0)
    upper = (lax.broadcasted_iota(jnp.int32, (LANES, LANES), 0) <= lax.broadcasted_iota(jnp.int32, (LANES, LANES), 1)).astype(bf16)
    lane = lax.broadcasted_iota(jnp.int32, (1, LANES), 1).astype(f32)
    slot_rows = lax.broadcasted_iota(jnp.int32, (capacity, LANES), 0)
    seen = jnp.zeros((num_experts, 1), f32)
    low = jnp.zeros((num_experts, capacity), f32)
    high = jnp.zeros((num_experts, capacity), f32)
    for blk in range(tok_count // LANES):
        span = slice(blk * LANES, (blk + 1) * LANES)
        ids = ids_ref[0, :, span]
        hot = jnp.where(expert == ids, 1.0, 0.0)
        count = jnp.dot(hot.astype(bf16), upper, preferred_element_type=f32) + seen
        slot = jnp.sum(hot * count, axis=0, keepdims=True).astype(jnp.int32) - 1
        seen = count[:, LANES - 1:]
        place_ref[0, :, span] = jnp.where(slot < capacity, ids * capacity + slot, -1)
        in_slot = jnp.where(slot_rows == slot, 1.0, 0.0).astype(bf16)
        dims = (((1,), (1,)), ((), ()))
        low = low + lax.dot_general((hot * lane).astype(bf16), in_slot, dims, preferred_element_type=f32)
        high = high + blk * lax.dot_general(hot.astype(bf16), in_slot, dims, preferred_element_type=f32)
    token_ref[0] = (high * LANES + low).astype(jnp.int32)


def routing(ids, num_experts, capacity):
    layers, _, tok_count = ids.shape
    row = pl.BlockSpec((1, 1, tok_count), lambda i: (i, 0, 0))
    return pl.pallas_call(
        functools.partial(routing_kernel, capacity),
        grid=(layers,),
        in_specs=[row],
        out_specs=[row, pl.BlockSpec((1, num_experts, capacity), lambda i: (i, 0, 0))],
        out_shape=[jax.ShapeDtypeStruct((layers, 1, tok_count), jnp.int32), jax.ShapeDtypeStruct((layers, num_experts, capacity), jnp.int32)],
        name="routing",
    )(ids)


def split_router(weight):
    hi = lax.reduce_precision(weight, 8, 7)
    mid = lax.reduce_precision(weight - hi, 8, 7)
    lo = lax.reduce_precision(weight - hi - mid, 8, 7)
    pad = jnp.zeros(weight.shape[:-1] + (LANES - 3 * weight.shape[-1],), weight.dtype)
    return jnp.concatenate([hi, mid, lo, pad], axis=-1).astype(bf16)


def attention_kernel(num_experts, x_ref, mask_ref, bias_ref, gain_ref, wq_ref, wk_ref, wv_ref, wo_ref, wr_ref, ids_ref, h1_ref, b_ref, gate_ref, ctx_ref):
    seq_len, model_dim = x_ref.shape[1:]
    num_heads = bias_ref.shape[0]
    head_dim = ctx_ref.shape[1] // num_heads
    gains = gain_ref[0]
    x = x_ref[0].astype(f32)
    a = (x * lax.rsqrt(jnp.mean(x * x, axis=-1, keepdims=True) + NORM_EPS) * gains[0:1]).astype(bf16)
    q = jnp.dot(a, wq_ref[0], preferred_element_type=f32).astype(bf16)
    k = jnp.dot(a, wk_ref[0], preferred_element_type=f32).astype(bf16)
    v = jnp.dot(a, wv_ref[0], preferred_element_type=f32).astype(bf16)
    mask_add = jnp.where(mask_ref[0] > 0, 0.0, NEG_BIG)
    first = lax.broadcasted_iota(jnp.int32, (seq_len, 2 * head_dim), 1) < head_dim
    zero = jnp.zeros((seq_len, 2 * head_dim), bf16)

    def probs(scores, head):
        scores = scores + bias_ref[head] + mask_add
        e = jnp.exp(scores - jnp.max(scores, axis=-1, keepdims=True))
        return (e * (1.0 / jnp.sum(e, axis=-1, keepdims=True))).astype(bf16)

    for pair in range(num_heads // 2):
        lanes = slice(2 * head_dim * pair, 2 * head_dim * (pair + 1))
        kp, vp = k[:, lanes], v[:, lanes]
        keys = jnp.concatenate([jnp.where(first, kp, zero), jnp.where(first, zero, kp)], axis=0)
        values = jnp.concatenate([jnp.where(first, vp, zero), jnp.where(first, zero, vp)], axis=0)
        s = lax.dot_general(q[:, lanes], keys, (((1,), (1,)), ((), ())), preferred_element_type=f32)
        p = jnp.concatenate([probs(s[:, :seq_len], 2 * pair), probs(s[:, seq_len:], 2 * pair + 1)], axis=1)
        ctx_ref[:, lanes] = jnp.dot(p, values, preferred_element_type=f32).astype(bf16)
    h1 = (x + jnp.dot(ctx_ref[...], wo_ref[0], preferred_element_type=f32)).astype(bf16)
    h1_ref[0] = h1
    h = h1.astype(f32)
    r = h * lax.rsqrt(jnp.mean(h * h, axis=-1, keepdims=True) + NORM_EPS) * gains[1:2]
    b = r.astype(bf16)
    b_ref[0] = b
    rest = r - b.astype(f32)
    mid = rest.astype(bf16)
    tail = (rest - mid.astype(f32)).astype(bf16)
    wr = wr_ref[0]
    lane = lax.broadcasted_iota(jnp.int32, (1, LANES), 1)
    part0 = jnp.dot(b, wr, preferred_element_type=f32)
    part1 = jnp.dot(mid, wr, preferred_element_type=f32)
    part2 = jnp.dot(tail, wr, preferred_element_type=f32)
    parts = part0 + jnp.where(lane < 2 * num_experts, part1, 0.0) + jnp.where(lane < num_experts, part2, 0.0)
    parts = parts.T
    logits = parts[:num_experts] + (parts[num_experts:2 * num_experts] + parts[2 * num_experts:3 * num_experts])
    e = jnp.exp(logits - jnp.max(logits, axis=0, keepdims=True))
    chosen = lax.broadcasted_iota(jnp.int32, (num_experts, seq_len), 0) == ids_ref[0, 0]
    gate_ref[0] = jnp.sum(jnp.where(chosen, e, 0.0), axis=0, keepdims=True) / jnp.sum(e, axis=0, keepdims=True)


def attention(layer, num_experts, x, mask, bias, ids, gains, wq, wk, wv, wo, wr):
    num_seqs, seq_len, model_dim = x.shape
    num_heads = bias.shape[0]
    inner = wq.shape[2]
    once = pl.Buffered(1)
    rows = pl.BlockSpec((1, seq_len, model_dim), lambda i: (i, 0, 0))
    line = pl.BlockSpec((1, 1, seq_len), lambda i: (i, 0, 0))

    def of_layer(array):
        return pl.BlockSpec((1,) + array.shape[1:], lambda i: (layer, 0, 0), pipeline_mode=once)

    flops = 2 * num_seqs * seq_len * (4 * model_dim * inner + 2 * seq_len * inner)
    return pl.pallas_call(
        functools.partial(attention_kernel, num_experts),
        grid=(num_seqs,),
        in_specs=[rows, line, pl.BlockSpec(bias.shape, lambda i: (0, 0, 0), pipeline_mode=once), of_layer(gains), of_layer(wq), of_layer(wk), of_layer(wv), of_layer(wo), of_layer(wr), pl.BlockSpec((1, 1, 1, seq_len), lambda i: (layer, i, 0, 0))],
        out_specs=[rows, rows, line],
        out_shape=[jax.ShapeDtypeStruct(x.shape, bf16), jax.ShapeDtypeStruct(x.shape, bf16), jax.ShapeDtypeStruct((num_seqs, 1, seq_len), f32)],
        scratch_shapes=[pltpu.VMEM((seq_len, inner), bf16)],
        compiler_params=pltpu.CompilerParams(vmem_limit_bytes=56 * 2**20),
        cost_estimate=pl.CostEstimate(flops=flops, bytes_accessed=8 * num_seqs * seq_len * model_dim, transcendentals=num_seqs * num_heads * seq_len * seq_len),
        name="attention",
    )(x, mask, bias, gains, wq, wk, wv, wo, wr, ids)


def exchange_kernel(layer, n, packed_ref, w_in_ref, w_out_ref, out_ref, rows, hid, up, down, load_sem, send_sem, recv_sem, ret_send, ret_recv, own_sem):
    local, _, cap, dim = rows.shape
    ff = up.shape[2]
    per = hid.shape[0] // cap
    me = lax.axis_index("ep")
    order = sorted(range(1, n), key=lambda k: abs(k - n // 2))

    def load(j):
        return (
            pltpu.make_async_copy(w_in_ref.at[layer, j], up.at[j % 2], load_sem.at[j % 2, 0]),
            pltpu.make_async_copy(w_out_ref.at[layer, j], down.at[j % 2], load_sem.at[j % 2, 1]),
        )

    def send(j, k):
        peer = lax.rem(me + k, n)
        return pltpu.make_async_remote_copy(
            src_ref=packed_ref.at[peer * local + j],
            dst_ref=rows.at[j, me],
            send_sem=send_sem.at[j, k],
            recv_sem=recv_sem.at[j, k],
            device_id={"ep": peer},
            device_id_type=MESH,
        )

    def send_back(j, k):
        peer = lax.rem(me + k, n)
        return pltpu.make_async_remote_copy(
            src_ref=rows.at[j, peer],
            dst_ref=out_ref.at[me * local + j],
            send_sem=ret_send.at[j, k],
            recv_sem=ret_recv.at[j, k],
            device_id={"ep": peer},
            device_id_type=MESH,
        )

    for c in load(0):
        c.start()
    barrier = pltpu.get_barrier_semaphore()
    for k in range(1, n):
        pl.semaphore_signal(barrier, inc=1, device_id={"ep": lax.rem(me + k, n)}, device_id_type=MESH)
    pl.semaphore_wait(barrier, n - 1)
    own_in = [pltpu.make_async_copy(packed_ref.at[me * local + j], rows.at[j, me], own_sem.at[0, j]) for j in range(local)]
    own_out = [pltpu.make_async_copy(rows.at[j, me], out_ref.at[me * local + j], own_sem.at[1, j]) for j in range(local)]
    for j in range(local):
        for k in order:
            send(j, k).start()
        own_in[j].start()
    for j in range(local):
        for c in load(j):
            c.wait()
        if j + 1 < local:
            for c in load(j + 1):
                c.start()
        own_in[j].wait()
        for k in order:
            send(j, k).wait_recv()

        @pl.loop(0, n // per)
        def _(i):
            x = rows[j, pl.ds(i * per, per)].reshape(per * cap, dim)

            @pl.loop(0, ff // dim)
            def _(c):
                cols = pl.ds(pl.multiple_of(c * dim, dim), dim)
                hid[:, cols] = jnp.maximum(jnp.dot(x, up[j % 2, :, cols], preferred_element_type=f32), 0.0).astype(bf16)

            @pl.loop(0, dim // 256)
            def _(c):
                cols = pl.ds(pl.multiple_of(c * 256, 256), 256)
                y = jnp.dot(hid[...], down[j % 2, :, cols], preferred_element_type=f32).astype(bf16)
                rows[j, pl.ds(i * per, per), :, cols] = y.reshape(per, cap, 256)

        for k in order:
            send_back(j, k).start()
        own_out[j].start()
    for j in range(local):
        for k in order:
            send(j, k).wait_send()
            send_back(j, k).wait_send()
            send_back(j, k).wait_recv()
        own_out[j].wait()


def exchange(layer, n, packed, w_in, w_out):
    num_experts, cap, dim = packed.shape
    local, ff = w_in.shape[1], w_in.shape[3]
    anywhere = pl.BlockSpec(memory_space=pl.ANY)
    return pl.pallas_call(
        functools.partial(exchange_kernel, layer, n),
        in_specs=[anywhere] * 3,
        out_specs=anywhere,
        out_shape=jax.ShapeDtypeStruct(packed.shape, bf16),
        scratch_shapes=[
            pltpu.VMEM((local, n, cap, dim), bf16),
            pltpu.VMEM((2 * cap, ff), bf16),
            pltpu.VMEM((2, dim, ff), bf16),
            pltpu.VMEM((2, ff, dim), bf16),
            pltpu.SemaphoreType.DMA((2, 2)),
            pltpu.SemaphoreType.DMA((local, n)),
            pltpu.SemaphoreType.DMA((local, n)),
            pltpu.SemaphoreType.DMA((local, n)),
            pltpu.SemaphoreType.DMA((local, n)),
            pltpu.SemaphoreType.DMA((2, local)),
        ],
        compiler_params=pltpu.CompilerParams(collective_id=layer, has_side_effects=True, vmem_limit_bytes=60 * 2**20),
        cost_estimate=pl.CostEstimate(flops=4 * n * local * cap * dim * ff, bytes_accessed=4 * local * dim * ff + 8 * num_experts * cap * dim, transcendentals=0),
        name="exchange%d" % layer,
    )(packed, w_in, w_out)


def solution(mesh):
    token_spec = P(('dp', 'ep'))
    n = mesh.shape['ep']

    def per_device(x_in, pad_mask, rel_bias, expert_idx, norm_scale, w_query, w_key, w_value, w_attn_out, w_router, w_in, w_out):
        num_seqs, seq_len, model_dim = x_in.shape
        tok_count = num_seqs * seq_len
        num_layers, _, num_experts = w_router.shape
        capacity = (CAP_FACTOR * tok_count + num_experts - 1) // num_experts
        place, slot_token = routing(expert_idx.reshape(num_layers, 1, tok_count), num_experts, capacity)
        ids = expert_idx.reshape(num_layers, num_seqs, 1, seq_len)
        mask = pad_mask.reshape(num_seqs, 1, seq_len)
        router = split_router(w_router)
        hidden = x_in
        for layer in range(num_layers):
            h1, b, gate = attention(layer, num_experts, hidden, mask, rel_bias, ids, norm_scale, w_query, w_key, w_value, w_attn_out, router)
            packed = jnp.take(b.reshape(tok_count, model_dim), slot_token[layer].reshape(-1), axis=0, mode='clip')
            back = exchange(layer, n, packed.reshape(num_experts, capacity, model_dim), w_in, w_out)
            spot = place[layer, 0]
            u = jnp.take(back.reshape(-1, model_dim), jnp.maximum(spot, 0), axis=0, mode='clip').astype(f32)
            h1 = h1.reshape(tok_count, model_dim).astype(f32)
            hidden = jnp.where(spot[:, None] >= 0, h1 + gate.reshape(-1, 1) * u, h1).astype(bf16).reshape(x_in.shape)
        return hidden

    return jax.shard_map(per_device, mesh=mesh, in_specs=(token_spec, token_spec, P(), P(None, ('dp', 'ep')), P(), P(), P(), P(), P(), P(), P(None, 'ep'), P(None, 'ep')), out_specs=token_spec, check_vma=False)
```

```python
import functools

import jax
import jax.numpy as jnp
from jax import lax
from jax.experimental import pallas as pl
from jax.experimental.pallas import tpu as pltpu
from jax.sharding import PartitionSpec as P

NORM_EPS = 1e-6
NEG_BIG = -1e9
CAP_FACTOR = 2
LANES = 128
SUBLANES = 8
MESH = pl.DeviceIdType.MESH
f32 = jnp.float32
bf16 = jnp.bfloat16


def routing_kernel(capacity, ids_ref, place_ref, token_ref):
    num_experts = token_ref.shape[1]
    tok_count = ids_ref.shape[2]
    expert = lax.broadcasted_iota(jnp.int32, (num_experts, LANES), 0)
    upper = (lax.broadcasted_iota(jnp.int32, (LANES, LANES), 0) <= lax.broadcasted_iota(jnp.int32, (LANES, LANES), 1)).astype(bf16)
    lane = lax.broadcasted_iota(jnp.int32, (1, LANES), 1).astype(f32)
    slot_rows = lax.broadcasted_iota(jnp.int32, (capacity, LANES), 0)
    seen = jnp.zeros((num_experts, 1), f32)
    found = jnp.zeros((capacity, 2 * num_experts), f32)
    for blk in range(tok_count // LANES):
        span = slice(blk * LANES, (blk + 1) * LANES)
        ids = ids_ref[0, :, span]
        hot = jnp.where(expert == ids, 1.0, 0.0)
        count = jnp.dot(hot.astype(bf16), upper, preferred_element_type=f32) + seen
        slot = jnp.sum(hot * count, axis=0, keepdims=True).astype(jnp.int32) - 1
        seen = count[:, LANES - 1:]
        place_ref[0, :, span] = jnp.where(slot < capacity, ids * capacity + slot, -1)
        in_slot = jnp.where(slot_rows == slot, 1.0, 0.0).astype(bf16)
        names = jnp.concatenate([hot * lane, hot * blk], axis=0).astype(bf16)
        found = found + lax.dot_general(in_slot, names, (((1,), (1,)), ((), ())), preferred_element_type=f32)
    found = found.T
    token_ref[0] = (found[num_experts:] * LANES + found[:num_experts]).astype(jnp.int32)


def routing(ids, num_experts, capacity):
    layers, _, tok_count = ids.shape
    row = pl.BlockSpec((1, 1, tok_count), lambda i: (i, 0, 0))
    return pl.pallas_call(
        functools.partial(routing_kernel, capacity),
        grid=(layers,),
        in_specs=[row],
        out_specs=[row, pl.BlockSpec((1, num_experts, capacity), lambda i: (i, 0, 0))],
        out_shape=[jax.ShapeDtypeStruct((layers, 1, tok_count), jnp.int32), jax.ShapeDtypeStruct((layers, num_experts, capacity), jnp.int32)],
        name="routing",
    )(ids)


def split_router(weight):
    hi = lax.reduce_precision(weight, 8, 7)
    mid = lax.reduce_precision(weight - hi, 8, 7)
    lo = lax.reduce_precision(weight - hi - mid, 8, 7)
    pad = jnp.zeros(weight.shape[:-1] + (LANES - 3 * weight.shape[-1],), weight.dtype)
    return jnp.concatenate([hi, mid, lo, pad], axis=-1).astype(bf16)


def combined(h1, u, gate, spot):
    return jnp.where(spot >= 0, h1 + gate * u, h1).astype(bf16)


def attention_kernel(num_experts, blended, *refs):
    refs = list(refs)
    if blended:
        u_ref, past_gate_ref, spot_ref = refs[:3]
        refs = refs[3:]
    x_ref, mask_ref, bias_ref, gain_ref, wq_ref, wk_ref, wv_ref, wo_ref, wr_ref, ids_ref, h1_ref, gate_ref, tiles_ref, ctx_ref = refs
    seq_len, model_dim = x_ref.shape[1:]
    num_heads = bias_ref.shape[0]
    head_dim = ctx_ref.shape[1] // num_heads
    chunks = model_dim // LANES
    gains = gain_ref[0]
    if blended:
        lines = jnp.concatenate([past_gate_ref[0], spot_ref[0].astype(f32), jnp.zeros((6, seq_len), f32)], axis=0).T
        x = combined(x_ref[0].astype(f32), u_ref[0].astype(f32), lines[:, 0:1], lines[:, 1:2]).astype(f32)
    else:
        x = x_ref[0].astype(f32)
    a = (x * lax.rsqrt(jnp.mean(x * x, axis=-1, keepdims=True) + NORM_EPS) * gains[0:1]).astype(bf16)
    q = jnp.dot(a, wq_ref[0], preferred_element_type=f32).astype(bf16)
    k = jnp.dot(a, wk_ref[0], preferred_element_type=f32).astype(bf16)
    v = jnp.dot(a, wv_ref[0], preferred_element_type=f32).astype(bf16)
    mask_add = jnp.where(mask_ref[0] > 0, 0.0, NEG_BIG)
    first = lax.broadcasted_iota(jnp.int32, (seq_len, 2 * head_dim), 1) < head_dim
    zero = jnp.zeros((seq_len, 2 * head_dim), bf16)

    def probs(scores, head):
        scores = scores + bias_ref[head] + mask_add
        e = jnp.exp(scores - jnp.max(scores, axis=-1, keepdims=True))
        return (e * (1.0 / jnp.sum(e, axis=-1, keepdims=True))).astype(bf16)

    for pair in range(num_heads // 2):
        lanes = slice(2 * head_dim * pair, 2 * head_dim * (pair + 1))
        kp, vp = k[:, lanes], v[:, lanes]
        keys = jnp.concatenate([jnp.where(first, kp, zero), jnp.where(first, zero, kp)], axis=0)
        values = jnp.concatenate([jnp.where(first, vp, zero), jnp.where(first, zero, vp)], axis=0)
        s = lax.dot_general(q[:, lanes], keys, (((1,), (1,)), ((), ())), preferred_element_type=f32)
        p = jnp.concatenate([probs(s[:, :seq_len], 2 * pair), probs(s[:, seq_len:], 2 * pair + 1)], axis=1)
        ctx_ref[:, lanes] = jnp.dot(p, values, preferred_element_type=f32).astype(bf16)
    h1 = (x + jnp.dot(ctx_ref[...], wo_ref[0], preferred_element_type=f32)).astype(bf16)
    h1_ref[0] = h1
    h = h1.astype(f32)
    r = h * lax.rsqrt(jnp.mean(h * h, axis=-1, keepdims=True) + NORM_EPS) * gains[1:2]
    for c in range(chunks):
        tiles_ref[pl.ds(c, seq_len, stride=SUBLANES), :] = r[:, c * LANES:(c + 1) * LANES]
    b = r.astype(bf16)
    rest = r - b.astype(f32)
    mid = rest.astype(bf16)
    tail = (rest - mid.astype(f32)).astype(bf16)
    wr = wr_ref[0]
    lane = lax.broadcasted_iota(jnp.int32, (1, LANES), 1)
    part0 = jnp.dot(b, wr, preferred_element_type=f32)
    part1 = jnp.dot(mid, wr, preferred_element_type=f32)
    part2 = jnp.dot(tail, wr, preferred_element_type=f32)
    parts = part0 + jnp.where(lane < 2 * num_experts, part1, 0.0) + jnp.where(lane < num_experts, part2, 0.0)
    parts = parts.T
    logits = parts[:num_experts] + (parts[num_experts:2 * num_experts] + parts[2 * num_experts:3 * num_experts])
    e = jnp.exp(logits - jnp.max(logits, axis=0, keepdims=True))
    chosen = lax.broadcasted_iota(jnp.int32, (num_experts, seq_len), 0) == ids_ref[0, 0]
    gate_ref[0] = jnp.sum(jnp.where(chosen, e, 0.0), axis=0, keepdims=True) / jnp.sum(e, axis=0, keepdims=True)


def attention(layer, num_experts, past, x, mask, bias, ids, gains, wq, wk, wv, wo, wr):
    num_seqs, seq_len, model_dim = x.shape
    num_heads = bias.shape[0]
    inner = wq.shape[2]
    once = pl.Buffered(1)
    rows = pl.BlockSpec((1, seq_len, model_dim), lambda i: (i, 0, 0))
    line = pl.BlockSpec((1, 1, seq_len), lambda i: (i, 0, 0))

    def of_layer(array):
        return pl.BlockSpec((1,) + array.shape[1:], lambda i: (layer, 0, 0), pipeline_mode=once)

    weights = [gains, wq, wk, wv, wo, wr]
    flops = 2 * num_seqs * seq_len * (4 * model_dim * inner + 2 * seq_len * inner)
    return pl.pallas_call(
        functools.partial(attention_kernel, num_experts, bool(past)),
        grid=(num_seqs,),
        in_specs=[rows, line, line][:len(past)]
        + [rows, line, pl.BlockSpec(bias.shape, lambda i: (0, 0, 0), pipeline_mode=once)]
        + [of_layer(w) for w in weights]
        + [pl.BlockSpec((1, 1, 1, seq_len), lambda i: (layer, i, 0, 0))],
        out_specs=[rows, line, pl.BlockSpec((seq_len * SUBLANES, LANES), lambda i: (i, 0))],
        out_shape=[jax.ShapeDtypeStruct(x.shape, bf16), jax.ShapeDtypeStruct((num_seqs, 1, seq_len), f32), jax.ShapeDtypeStruct((num_seqs * seq_len * SUBLANES, LANES), f32)],
        scratch_shapes=[pltpu.VMEM((seq_len, inner), bf16)],
        compiler_params=pltpu.CompilerParams(vmem_limit_bytes=56 * 2**20),
        cost_estimate=pl.CostEstimate(flops=flops, bytes_accessed=8 * num_seqs * seq_len * model_dim, transcendentals=num_seqs * num_heads * seq_len * seq_len),
        name="attention%d" % layer,
    )(*past, x, mask, bias, *weights, ids)


def exchange_kernel(layer, n, token_ref, tiles_ref, w_in_ref, w_out_ref, out_ref, src, stage, outgoing, rows, hid, up, down, load_sem, send_sem, recv_sem, ret_send, ret_recv, own_sem):
    local, _, cap, dim = rows.shape
    ff = up.shape[1]
    per = hid.shape[0] // cap
    me = lax.axis_index("ep")
    order = sorted(range(1, n), key=lambda k: abs(k - n // 2))
    fetch = pltpu.make_async_copy(tiles_ref, src, load_sem.at[2])

    def load(j):
        return (
            pltpu.make_async_copy(w_in_ref.at[layer, j], up, load_sem.at[0]),
            pltpu.make_async_copy(w_out_ref.at[layer, j], down, load_sem.at[1]),
        )

    def send(j, k):
        peer = lax.rem(me + k, n)
        return pltpu.make_async_remote_copy(
            src_ref=outgoing.at[j % 2, k],
            dst_ref=rows.at[j, me],
            send_sem=send_sem.at[j, k],
            recv_sem=recv_sem.at[j, k],
            device_id={"ep": peer},
            device_id_type=MESH,
        )

    def send_back(j, k):
        peer = lax.rem(me + k, n)
        return pltpu.make_async_remote_copy(
            src_ref=rows.at[j, peer],
            dst_ref=out_ref.at[me * local + j],
            send_sem=ret_send.at[j, k],
            recv_sem=ret_recv.at[j, k],
            device_id={"ep": peer},
            device_id_type=MESH,
        )

    def gather(j, k, dst):
        base = (lax.rem(me + k, n) * local + j) * cap

        @pl.loop(0, cap // 16)
        def _(i):
            for sub in range(16):
                stage[pl.ds(pl.multiple_of((i * 16 + sub) * SUBLANES, SUBLANES), SUBLANES), :] = src[token_ref[base + i * 16 + sub]]

        for c in range(dim // LANES):
            dst[:, c * LANES:(c + 1) * LANES] = stage[pl.ds(c, cap, stride=SUBLANES), :].astype(bf16)

    def kth(m):
        half = (m + 1) // 2
        return n // 2 + jnp.where(m % 2 == 0, half, -half)

    def dispatch(j):
        if j >= 2:
            for k in order:
                send(j - 2, k).wait_send()
        gather(j, n // 2, outgoing.at[j % 2, n // 2])

        @pl.loop(1, n - 1)
        def _(m):
            gather(j, kth(m), outgoing.at[j % 2, kth(m)])
            send(j, kth(m - 1)).start()

        gather(j, 0, rows.at[j, me])
        send(j, order[-1]).start()

    def expert(j):
        for k in order:
            send(j, k).wait_recv()
        for c in load(j):
            c.wait()

        @pl.loop(0, n // per)
        def _(i):
            x = rows[j, pl.ds(i * per, per)].reshape(per * cap, dim)

            @pl.loop(0, ff // dim)
            def _(c):
                cols = pl.ds(pl.multiple_of(c * dim, dim), dim)
                hid[:, cols] = jnp.maximum(jnp.dot(x, up[:, cols], preferred_element_type=f32), 0.0).astype(bf16)

            @pl.loop(0, dim // 256)
            def _(c):
                cols = pl.ds(pl.multiple_of(c * 256, 256), 256)
                y = jnp.dot(hid[...], down[:, cols], preferred_element_type=f32).astype(bf16)
                rows[j, pl.ds(i * per, per), :, cols] = y.reshape(per, cap, 256)

        if j + 1 < local:
            for c in load(j + 1):
                c.start()
        for k in order:
            send_back(j, k).start()
        own_out[j].start()

    own_out = [pltpu.make_async_copy(rows.at[j, me], out_ref.at[me * local + j], own_sem.at[j]) for j in range(local)]
    fetch.start()
    barrier = pltpu.get_barrier_semaphore()
    for k in range(1, n):
        pl.semaphore_signal(barrier, inc=1, device_id={"ep": lax.rem(me + k, n)}, device_id_type=MESH)
    pl.semaphore_wait(barrier, n - 1)
    fetch.wait()
    for c in load(0):
        c.start()
    for j in range(local):
        dispatch(j)
        if j >= 2:
            expert(j - 2)
    for j in range(max(local - 2, 0), local):
        expert(j)
    for j in range(local):
        for k in order:
            if j >= local - 2:
                send(j, k).wait_send()
            send_back(j, k).wait_send()
            send_back(j, k).wait_recv()
        own_out[j].wait()


def exchange(layer, n, slot_token, tiles, w_in, w_out):
    num_experts, cap = slot_token.shape
    local, dim, ff = w_in.shape[1:]
    anywhere = pl.BlockSpec(memory_space=pl.ANY)
    dma = pltpu.SemaphoreType.DMA
    return pl.pallas_call(
        functools.partial(exchange_kernel, layer, n),
        in_specs=[pl.BlockSpec(memory_space=pltpu.SMEM)] + [anywhere] * 3,
        out_specs=anywhere,
        out_shape=jax.ShapeDtypeStruct((num_experts, cap, dim), bf16),
        scratch_shapes=[
            pltpu.VMEM((tiles.shape[0] // SUBLANES, SUBLANES, LANES), f32),
            pltpu.VMEM((cap * SUBLANES, LANES), f32),
            pltpu.VMEM((2, n, cap, dim), bf16),
            pltpu.VMEM((local, n, cap, dim), bf16),
            pltpu.VMEM((2 * cap, ff), bf16),
            pltpu.VMEM((dim, ff), bf16),
            pltpu.VMEM((ff, dim), bf16),
            dma((3,)),
            dma((local, n)),
            dma((local, n)),
            dma((local, n)),
            dma((local, n)),
            dma((local,)),
        ],
        compiler_params=pltpu.CompilerParams(collective_id=layer, has_side_effects=True, vmem_limit_bytes=62 * 2**20),
        cost_estimate=pl.CostEstimate(flops=4 * n * local * cap * dim * ff, bytes_accessed=4 * local * dim * ff + 8 * num_experts * cap * dim, transcendentals=0),
        name="exchange%d" % layer,
    )(slot_token.reshape(-1), tiles.reshape(-1, SUBLANES, LANES), w_in, w_out)


def solution(mesh):
    token_spec = P(('dp', 'ep'))
    n = mesh.shape['ep']

    def per_device(x_in, pad_mask, rel_bias, expert_idx, norm_scale, w_query, w_key, w_value, w_attn_out, w_router, w_in, w_out):
        num_seqs, seq_len, model_dim = x_in.shape
        tok_count = num_seqs * seq_len
        num_layers, _, num_experts = w_router.shape
        capacity = (CAP_FACTOR * tok_count + num_experts - 1) // num_experts
        place, slot_token = routing(expert_idx.reshape(num_layers, 1, tok_count), num_experts, capacity)
        ids = expert_idx.reshape(num_layers, num_seqs, 1, seq_len)
        mask = pad_mask.reshape(num_seqs, 1, seq_len)
        router = split_router(w_router)
        hidden, past = x_in, ()
        for layer in range(num_layers):
            h1, gate, tiles = attention(layer, num_experts, past, hidden, mask, rel_bias, ids, norm_scale, w_query, w_key, w_value, w_attn_out, router)
            back = exchange(layer, n, slot_token[layer], tiles, w_in, w_out)
            spot = place[layer, 0]
            u = jnp.take(back.reshape(-1, model_dim), jnp.maximum(spot, 0), axis=0, mode='clip')
            hidden, past = h1, (u.reshape(x_in.shape), gate, spot.reshape(num_seqs, 1, seq_len))
        shape = (num_seqs, seq_len, 1)
        return combined(h1.astype(f32), past[0].astype(f32), gate.reshape(shape), spot.reshape(shape))

    return jax.shard_map(per_device, mesh=mesh, in_specs=(token_spec, token_spec, P(), P(None, ('dp', 'ep')), P(), P(), P(), P(), P(), P(), P(None, 'ep'), P(None, 'ep')), out_specs=token_spec, check_vma=False)
```
